32 devices in a mesh: len: 2 (over x), wid: 4 (over z), dep: 4 (over y, core).
Axes of the slice: x: 2, y: 2, z: 4, core: 2. Of those that a mesh axis runs over, the one named last changes fastest.
Arguments:
- coords: float32 [3, 32768], P(None, ('len', 'wid', 'dep')), may hold values from -3 to 3
- velocity: float32 [3, 32768], P(None, ('len', 'wid', 'dep')), may hold values from -6 to 6
- node_mass: float32 [32768], P(('len', 'wid', 'dep')), may hold values from 0.5 to 2
- corner_nodes: int32 [4, 32768], P(None, ('len', 'wid', 'dep')), may hold values from 0 to 1151, as said below
- shape_grad: float32 [8, 32768], P(None, ('len', 'wid', 'dep')), may hold values from -5 to 5
- frame_angles: float32 [2, 32768], P(None, ('len', 'wid', 'dep')), may hold values from -3.140625 to 3.140625
- volume: float32 [32768], P(('len', 'wid', 'dep')), may hold values from 0.5 to 2
- stress: float32 [3, 32768], P(None, ('len', 'wid', 'dep')), may hold values from -5 to 5
- send_nodes: int32 [32, 16, 256], P(('len', 'wid', 'dep')), may hold values from 0 to 1023
- tile_count: int32 [32], P(('len', 'wid', 'dep')), may hold values from 1 to 4, as said below
- tile_nodes: int32 [128, 128], P(('len', 'wid', 'dep')), may hold values from 0 to 4095
- tile_facets: int32 [4, 128, 128], P(None, ('len', 'wid', 'dep')), may hold values from 0 to 4095
- pair_mask: int32 [128, 128, 128], P(('len', 'wid', 'dep')), may hold values 0 or 1
Outputs:
- coords_out: float32 [3, 32768], P(None, ('len', 'wid', 'dep'))
- velocity_out: float32 [3, 32768], P(None, ('len', 'wid', 'dep'))
- stress_out: float32 [3, 32768], P(None, ('len', 'wid', 'dep'))
The draws below stay inside these ranges and needn't reach their ends.
Inputs may be any that keep to these rules, and one draw needn't show every extreme that they name: `corner_nodes`: for the element at device-local position i (i = e mod 1024), every entry lies from (i // 128) * 128 to (i // 128) * 128 + 2 * 128 - 1. An entry j below 1024 names the element device's own node j; an entry 1024 + i names node i of the next device in the order len, wid, dep, the last device's next being the first. `send_nodes`: entry [p, g, k] is a node of device p, by its local number, sent to device g of p's slab; nodes may repeat. `tile_count`: some device has 4 live tiles in every draw; a device's tiles at and past its count are not used. `tile_nodes`: slot g * 256 + k of the tile's device is slot k of what device g of its slab sends it. `tile_facets`: slots as for tile_nodes, one for each of a facet's four corners.
All inputs are finite; a program needn't handle non-finite values. No bound on the sum of `pair_mask` on one device may be relied on, other than what follows from the above.
Results may differ from the reference program's by a relative error of at most 0.0003.
Values sent between devices are 32-bit elements; how exact they have to be, the bound alone decides.
A program may use at most 64 MiB of HBM per device.

```python
import math
import jax
import jax.numpy as jnp
from jax import lax

ELEM_DEV = 1024
NODE_DEV = 1024
RIM = 128
SEND_CAP = 256
TILE_CAP = 4
TILE_NODE = 128
TILE_FACET = 128
STEPS = 2
GROUP = 16
ELEMS = 32768
NODES = 32768
TILES = 128
N_LEN = 2
N_WID = 4
N_DEP = 4
DEVICES = 32


def draw_tile_count(key, part):
    key_heavy = jax.random.fold_in(key, 11)
    key_light = jax.random.fold_in(key, 12)
    key_chosen = jax.random.fold_in(key, 13)
    is_heavy = jax.random.randint(key_heavy, (DEVICES,), 0, 8) == 0
    light_count = jax.random.randint(key_light, (DEVICES,), 1, max(TILE_CAP // 4, 1) + 1)
    counts = jnp.where(is_heavy, TILE_CAP, light_count)
    chosen = jax.random.randint(key_chosen, (), 0, DEVICES)
    return jnp.where(jnp.arange(DEVICES) == chosen, TILE_CAP, counts).astype(jnp.int32)


def draw_corner_nodes(key, part):
    key_offset = jax.random.fold_in(key, 21)
    position = jnp.arange(ELEMS, dtype=jnp.int32) % ELEM_DEV
    block_start = position // RIM * RIM
    offset = jax.random.randint(key_offset, (4, ELEMS), 0, 2 * RIM)
    return (block_start[None, :] + offset).astype(jnp.int32)


def set_ends(drawn, key, least, high):
    longest = drawn.shape.index(max(drawn.shape))
    spots = []
    for shift in (0, 1):
        where = [jax.random.randint(jax.random.fold_in(key, axis), (), 0, length) for axis, length in enumerate(drawn.shape)]
        where[longest] = (where[longest] + shift) % drawn.shape[longest]
        spots.append(tuple(where))
    return drawn.at[spots[0]].set(least).at[spots[1]].set(high)


def steps_of(stream_key, extent, cuts, low, largest):
    level = 1.0
    for dim, shards_of in cuts:
        steps = jax.random.uniform(jax.random.fold_in(jax.random.fold_in(stream_key, 6), dim), (shards_of,), jnp.float32, low / len(cuts), largest / len(cuts))
        level = level * jnp.repeat(jnp.exp(steps), extent[dim] // shards_of).reshape((-1,) + (1,) * (len(extent) - 1 - dim))
    return level


def bell_draw(stream_key, shape, deviation, bound, shards=(), kind=jnp.bfloat16):
    values = deviation * jax.random.normal(stream_key, shape, jnp.float32)
    if shards:
        values = values * steps_of(stream_key, shape, shards, -0.22, 0.18)
    return jnp.clip(values, -bound, bound).astype(kind)


def setup_inputs(seed: int = 0) -> dict:
    splits = jax.random.split(jax.random.key(seed), 14)
    coords = bell_draw(splits[0], (3, NODES), 0.5, 3.0, ((1, 32),), jnp.float32)
    velocity = bell_draw(splits[1], (3, NODES), 1.0, 6.0, ((1, 32),), jnp.float32)
    node_mass = jnp.clip(jnp.exp(math.log(2.0) - 1.3862944 * jax.random.uniform(splits[2], (NODES,), jnp.float32) ** steps_of(splits[2], (NODES,), ((0, 32),), -0.2, 0.2)), 0.5, 2.0)
    corner_nodes = draw_corner_nodes(jax.random.fold_in(splits[13], 71), 0)
    shape_grad = bell_draw(splits[4], (8, ELEMS), 1.0, 5.0, ((1, 32),), jnp.float32)
    frame_angles = jnp.clip(jax.random.uniform(splits[5], (2, ELEMS), jnp.float32, -3.140625, 3.140625), -3.140625, 3.140625)
    volume = jnp.clip(jnp.exp(math.log(2.0) - 1.3862944 * jax.random.uniform(splits[6], (ELEMS,), jnp.float32) ** steps_of(splits[6], (ELEMS,), ((0, 32),), -0.2, 0.2)), 0.5, 2.0)
    stress = bell_draw(splits[7], (3, ELEMS), 1.0, 5.0, ((1, 32),), jnp.float32)
    send_nodes = set_ends(jax.random.randint(splits[8], (DEVICES, GROUP, SEND_CAP), 0, NODE_DEV), jax.random.fold_in(splits[8], 1), 0, NODE_DEV - 1).astype(jnp.int32)
    tile_count = draw_tile_count(jax.random.fold_in(splits[13], 71), 0)
    tile_nodes = set_ends(jax.random.randint(splits[10], (TILES, TILE_NODE), 0, GROUP * SEND_CAP), jax.random.fold_in(splits[10], 1), 0, (GROUP * SEND_CAP) - 1).astype(jnp.int32)
    tile_facets = set_ends(jax.random.randint(splits[11], (4, TILES, TILE_FACET), 0, GROUP * SEND_CAP), jax.random.fold_in(splits[11], 1), 0, (GROUP * SEND_CAP) - 1).astype(jnp.int32)
    pair_mask = set_ends((jax.random.randint(splits[12], (TILES, TILE_NODE, TILE_FACET), 0, 2) < 1).astype(jnp.int32), jax.random.fold_in(splits[12], 1), 0, 1)
    return {"coords": coords, "velocity": velocity, "node_mass": node_mass, "corner_nodes": corner_nodes, "shape_grad": shape_grad, "frame_angles": frame_angles, "volume": volume, "stress": stress, "send_nodes": send_nodes, "tile_count": tile_count, "tile_nodes": tile_nodes, "tile_facets": tile_facets, "pair_mask": pair_mask}


TIME_STEP = 0.1
YOUNG_MOD = 1.0
POISSON = 0.3
HOURGLASS = 0.1
RADIUS_SQ = 1.0
STIFFNESS = 0.1
DAMPING = 0.05


def frame_vectors(frame_angles):
    polar_angle = frame_angles[0]
    azimuth = frame_angles[1]
    axis_one = jnp.stack([jnp.cos(polar_angle) * jnp.cos(azimuth), jnp.cos(polar_angle) * jnp.sin(azimuth), -jnp.sin(polar_angle)])
    axis_two = jnp.stack([-jnp.sin(azimuth), jnp.cos(azimuth), jnp.zeros_like(azimuth)])
    return axis_one, axis_two


def element_forces(corner_vel, shape_grad, axis_one, axis_two, volume, stress):
    grad_x = shape_grad[:4]
    grad_y = shape_grad[4:]
    along_one = jnp.sum(axis_one[:, None, :] * corner_vel, axis=0)
    along_two = jnp.sum(axis_two[:, None, :] * corner_vel, axis=0)
    rate_xx = jnp.sum(grad_x * along_one, axis=0)
    rate_yy = jnp.sum(grad_y * along_two, axis=0)
    rate_xy = jnp.sum(grad_y * along_one + grad_x * along_two, axis=0)
    factor = TIME_STEP * YOUNG_MOD / (1.0 - POISSON * POISSON)
    sigma_xx = stress[0] + factor * (rate_xx + POISSON * rate_yy)
    sigma_yy = stress[1] + factor * (POISSON * rate_xx + rate_yy)
    sigma_xy = stress[2] + factor * 0.5 * (1.0 - POISSON) * rate_xy
    hourglass_mode = jnp.array([1.0, -1.0, 1.0, -1.0], jnp.float32)[:, None]
    hourglass_rate = jnp.sum(hourglass_mode[None] * corner_vel, axis=1)
    force_one = -volume * (grad_x * sigma_xx + grad_y * sigma_xy)
    force_two = -volume * (grad_y * sigma_yy + grad_x * sigma_xy)
    corner_force = axis_one[:, None] * force_one[None] + axis_two[:, None] * force_two[None] - HOURGLASS * volume * hourglass_mode[None] * hourglass_rate[:, None]
    return corner_force, jnp.stack([sigma_xx, sigma_yy, sigma_xy])


def tile_forces(node_coordinates, node_velocities, corner_pos, corner_vel, pair_bits, live_row):
    facet_centroid = 0.25 * jnp.sum(corner_pos, axis=1)
    centroid_velocity = 0.25 * jnp.sum(corner_vel, axis=1)
    inner_product = jnp.einsum("ywq,ywk->wqk", node_coordinates, facet_centroid, precision=lax.Precision.HIGHEST)
    distance = jnp.sum(node_coordinates * node_coordinates, axis=0)[:, :, None] + jnp.sum(facet_centroid * facet_centroid, axis=0)[:, None, :] - 2.0 * inner_product
    corner_weight = pair_bits.astype(jnp.float32) * live_row[:, None, None] * jnp.maximum(RADIUS_SQ - distance, 0.0)
    row_sum = jnp.sum(corner_weight, axis=2)
    col_sum = jnp.sum(corner_weight, axis=1)
    gathered_positions = jnp.einsum("yml,mjl->ymj", facet_centroid, corner_weight, precision=lax.Precision.HIGHEST)
    gathered_velocities = jnp.einsum("yml,mjl->ymj", centroid_velocity, corner_weight, precision=lax.Precision.HIGHEST)
    node_force = STIFFNESS * (row_sum * node_coordinates - gathered_positions) - DAMPING * (row_sum * node_velocities - gathered_velocities)
    outgoing_positions = jnp.einsum("ewo,woj->ewj", node_coordinates, corner_weight, precision=lax.Precision.HIGHEST)
    outgoing_velocities = jnp.einsum("ewo,woj->ewj", node_velocities, corner_weight, precision=lax.Precision.HIGHEST)
    facet_force = STIFFNESS * (outgoing_positions - col_sum * facet_centroid) - DAMPING * (outgoing_velocities - col_sum * centroid_velocity)
    return node_force, -0.25 * facet_force


def reference(coords, velocity, node_mass, corner_nodes, shape_grad, frame_angles, volume, stress, send_nodes, tile_count, tile_nodes, tile_facets, pair_mask):
    group_size = N_WID * N_DEP
    owners = jnp.arange(ELEMS, dtype=jnp.int32) // ELEM_DEV
    node_of = ((owners[None, :] * NODE_DEV + corner_nodes) % NODES).astype(jnp.int32)
    axis_one, axis_two = frame_vectors(frame_angles)
    sources = jnp.arange(DEVICES, dtype=jnp.int32)
    global_send = (sources[:, None, None] * NODE_DEV + send_nodes).astype(jnp.int32)
    by_source = global_send.reshape(N_LEN, group_size, group_size, SEND_CAP)
    slot_node = jnp.transpose(by_source, (0, 2, 1, 3)).reshape(DEVICES, group_size * SEND_CAP)
    nodes_three = tile_nodes.reshape(DEVICES, TILE_CAP, TILE_NODE)
    node_ids = slot_node[sources[:, None, None], nodes_three]
    facets_four = jnp.transpose(tile_facets.reshape(4, DEVICES, TILE_CAP, TILE_FACET), (1, 0, 2, 3))
    facet_ids = slot_node[sources[:, None, None, None], facets_four]
    live_tiles = (jnp.arange(TILE_CAP, dtype=jnp.int32)[None, :] < tile_count[:, None]).astype(jnp.float32)
    pair_bits = pair_mask.reshape(DEVICES, TILE_CAP, TILE_NODE, TILE_FACET)
    for repeat in range(STEPS):
        corner_force, stress = element_forces(velocity[:, node_of], shape_grad, axis_one, axis_two, volume, stress)
        internal = jnp.zeros((3, NODES), jnp.float32).at[:, node_of].add(corner_force)

        def per_device(pieces, coords=coords, velocity=velocity):
            ids_node, ids_facet, bit_rows, live_row = pieces
            return tile_forces(coords[:, ids_node], velocity[:, ids_node], coords[:, ids_facet], velocity[:, ids_facet], bit_rows, live_row)

        node_force, facet_share = lax.map(per_device, (node_ids, facet_ids, pair_bits, live_tiles))
        node_force = jnp.transpose(node_force, (1, 0, 2, 3))
        facet_share = jnp.transpose(facet_share, (1, 0, 2, 3))
        contact = jnp.zeros((3, NODES), jnp.float32).at[:, node_ids].add(node_force)
        for corner in range(4):
            contact = contact.at[:, facet_ids[:, corner]].add(facet_share)
        velocity = velocity + TIME_STEP * (internal + contact) / node_mass
        coords = coords + TIME_STEP * velocity
    return coords, velocity, stress
```

```python
import functools

import jax
import jax.numpy as jnp
from jax import lax
from jax.experimental import pallas as pl
from jax.experimental.pallas import tpu as pltpu
from jax.sharding import PartitionSpec as P

STEPS = 2
TIME_STEP = 0.1
YOUNG_MOD = 1.0
POISSON = 0.3
HOURGLASS = 0.1
RADIUS_SQ = 1.0
STIFFNESS = 0.1
DAMPING = 0.05

LANES = 128
OUT_ROWS = 12
BACK_ROWS = 6
MESH = pl.DeviceIdType.MESH
F32 = jnp.float32
BF16 = jnp.bfloat16


def two_parts(values):
    first = values.astype(BF16)
    return first, (values - first.astype(F32)).astype(BF16)


def lane_take(table, low):
    return jnp.take_along_axis(table, low, axis=1, mode="promise_in_bounds")


def nt_dot(left, right):
    return lax.dot_general(left, right, (((1,), (1,)), ((), ())), preferred_element_type=F32)


def nn_dot(left, right):
    return lax.dot_general(left, right, (((1,), (0,)), ((), ())), preferred_element_type=F32)


def kernel(
    sizes,
    coords_in, velocity_in, mass_in, corner_in, grad_in, angles_in, volume_in, stress_in,
    send_in, count_in, nodes_in, facets_in, mask_in,
    coords_out, velocity_out, stress_out,
    pos, vel, corner, grad, stress, angle, slot_ids, tile_ids, win_hot, tile_hot, node_hot,
    win_rows, tile_lhs, node_lhs,
    send_buf, recv_buf, back_buf, answer_buf, ghost_send, ghost_recv, rim_send, rim_recv,
    out_send_sem, out_recv_sem, back_send_sem, back_recv_sem, edge_send_sem, edge_recv_sem,
):
    n_len, n_wid, n_dep = sizes
    group = n_wid * n_dep
    devices = n_len * group
    rows = coords_in.shape[1] // LANES
    halves = send_in.shape[2] // LANES
    tiles = nodes_in.shape[0]
    my_len = lax.axis_index("len")
    my_place = lax.axis_index("wid") * n_dep + lax.axis_index("dep")
    my_id = my_len * group + my_place

    def by_id(p):
        return (p // group, (p % group) // n_dep, p % n_dep)

    def partner(d):
        g = lax.rem(my_place + d, group)
        return g, (my_len, g // n_dep, lax.rem(g, n_dep))

    before = by_id(lax.rem(my_id + devices - 1, devices))
    after = by_id(lax.rem(my_id + 1, devices))

    barrier = pltpu.get_barrier_semaphore()
    for d in range(1, group):
        pl.semaphore_signal(barrier, inc=1, device_id=partner(d)[1], device_id_type=MESH)
    pl.semaphore_signal(barrier, inc=1, device_id=before, device_id_type=MESH)
    pl.semaphore_signal(barrier, inc=1, device_id=after, device_id_type=MESH)

    for i in range(rows):
        cols = pl.ds(i * LANES, LANES)
        pos[pl.ds(i, 3, stride=rows), :] = coords_in[:, cols]
        for k in range(3):
            vel[pl.ds(k * 2 * rows + i, 1), :] = velocity_in[pl.ds(k, 1), cols]
        stress[pl.ds(i, 3, stride=rows), :] = stress_in[:, cols]
        corner[pl.ds(i, 4, stride=rows), :] = corner_in[:, cols]
        grad[pl.ds(i, 8, stride=rows), :] = grad_in[:, cols]
        angle[pl.ds(i, 2, stride=rows), :] = angles_in[:, cols]
    tile_rows = tile_ids.shape[0]
    tile_ids[...] = jnp.zeros_like(tile_ids)
    tile_ids[pl.ds(0, tiles), :] = nodes_in[...]
    for a in range(4):
        tile_ids[pl.ds((a + 1) * tiles, tiles), :] = facets_in[a]

    def velocity_rows(k):
        return vel[pl.ds(k * 2 * rows, rows), :]

    def edge_copy(step, which):
        src, dst, target = ((ghost_send, ghost_recv, before), (rim_send, rim_recv, after))[which]
        return pltpu.make_async_remote_copy(
            src_ref=src.at[step], dst_ref=dst.at[step],
            send_sem=edge_send_sem.at[step, which], recv_sem=edge_recv_sem.at[step, which],
            device_id=target, device_id_type=MESH,
        )

    def group_copy(step, d, back):
        g, target = partner(d)
        if back:
            src, dst, ss, rs, n = back_buf, answer_buf, back_send_sem, back_recv_sem, BACK_ROWS
        else:
            src, dst, ss, rs, n = send_buf, recv_buf, out_send_sem, out_recv_sem, OUT_ROWS
        return pltpu.make_async_remote_copy(
            src_ref=src.at[step, g], dst_ref=dst.at[step, my_place],
            send_sem=ss.at[step, d - 1], recv_sem=rs.at[step, d - 1],
            device_id=target, device_id_type=MESH,
        )

    def fill_ghosts(step):
        for k in range(3):
            ghost_send[step, pl.ds(k, 1), :] = vel[pl.ds(k * 2 * rows, 1), :]

    def fill_slots(step):
        tables = [pos[pl.ds(k * rows, rows), :] for k in range(3)]
        tables += [velocity_rows(k) for k in range(3)]
        for half in range(halves):
            ids = send_in[0, :, pl.ds(half * LANES, LANES)]
            low, high = ids & (LANES - 1), ids >> 7
            for c in range(6):
                found = jnp.zeros(ids.shape, F32)
                for h in range(rows):
                    row = jnp.broadcast_to(tables[c][h : h + 1], ids.shape)
                    found = jnp.where(high == h, lane_take(row, low), found)
                send_buf[step, :, c * halves + half, :] = found

    fill_ghosts(0)
    fill_slots(0)
    pl.semaphore_wait(barrier, group + 1)

    sub = lax.broadcasted_iota(jnp.int32, (LANES, LANES), 0)
    for step in range(STEPS):
        edge_copy(step, 0).start()
        for d in range(1, group):
            group_copy(step, d, False).start()
        recv_buf[step, my_place] = send_buf[step, my_place]

        if step == 0:
            first_row = lax.broadcasted_iota(jnp.int32, (rows, LANES), 0) * LANES
            corner_low, corner_far = [], []
            for a in range(4):
                local = corner[pl.ds(a * rows, rows), :] - first_row
                corner_low.append(local & (LANES - 1))
                corner_far.append(local >= LANES)
                for i in range(rows):
                    hot = (sub == corner_low[a][i : i + 1]).astype(F32).astype(BF16)
                    win_hot[i, :, pl.ds(a * LANES, LANES)] = hot
            polar, azim = angle[pl.ds(0, rows), :], angle[pl.ds(rows, rows), :]
            cos_p, sin_p, cos_a, sin_a = jnp.cos(polar), jnp.sin(polar), jnp.cos(azim), jnp.sin(azim)
            one = (cos_p * cos_a, cos_p * sin_a, -sin_p)
            two = (-sin_a, cos_a)
            volume = volume_in[...]
            mass = mass_in[...]
            gx = [grad[pl.ds(a * rows, rows), :] for a in range(4)]
            gy = [grad[pl.ds((4 + a) * rows, rows), :] for a in range(4)]

        edge_copy(step, 0).wait_recv()
        for k in range(3):
            vel[pl.ds(k * 2 * rows + rows, 1), :] = ghost_recv[step, pl.ds(k, 1), :]
        corner_vel = []
        for k in range(3):
            near = velocity_rows(k)
            far = vel[pl.ds(k * 2 * rows + 1, rows), :]
            corner_vel.append([
                jnp.where(corner_far[a], lane_take(far, corner_low[a]), lane_take(near, corner_low[a]))
                for a in range(4)
            ])
        xx = yy = xy = jnp.zeros((rows, LANES), F32)
        for a in range(4):
            u = sum(one[k] * corner_vel[k][a] for k in range(3))
            w = sum(two[k] * corner_vel[k][a] for k in range(2))
            xx += gx[a] * u
            yy += gy[a] * w
            xy += gy[a] * u + gx[a] * w
        factor = TIME_STEP * YOUNG_MOD / (1.0 - POISSON * POISSON)
        sxx = stress[pl.ds(0, rows), :] + factor * (xx + POISSON * yy)
        syy = stress[pl.ds(rows, rows), :] + factor * (POISSON * xx + yy)
        sxy = stress[pl.ds(2 * rows, rows), :] + factor * 0.5 * (1.0 - POISSON) * xy
        stress[pl.ds(0, rows), :] = sxx
        stress[pl.ds(rows, rows), :] = syy
        stress[pl.ds(2 * rows, rows), :] = sxy
        hour = [
            HOURGLASS * volume
            * (corner_vel[k][0] - corner_vel[k][1] + corner_vel[k][2] - corner_vel[k][3])
            for k in range(3)
        ]
        for a in range(4):
            f1 = -volume * (gx[a] * sxx + gy[a] * sxy)
            f2 = -volume * (gy[a] * syy + gx[a] * sxy)
            for k in range(3):
                force = one[k] * f1 - (1.0 if a % 2 == 0 else -1.0) * hour[k]
                if k < 2:
                    force += two[k] * f2
                first = force.astype(BF16).astype(F32)
                for part, value in enumerate((first, force - first)):
                    for side in range(2):
                        keep = corner_far[a] if side else jnp.logical_not(corner_far[a])
                        win_rows[a, pl.ds(part * 8 + k * 2 + side, rows, stride=16), :] = jnp.where(
                            keep, value, 0.0
                        )
        for i in range(rows):
            left = jnp.concatenate(
                [win_rows[a, pl.ds(i * 16, 16), :].astype(BF16) for a in range(4)], axis=1
            )
            summed = nt_dot(left, win_hot[i])
            rim_send[step, pl.ds(i * 8, 8), :] = summed[:8] + summed[8:]
        edge = pltpu.make_async_remote_copy(
            src_ref=rim_send.at[step, pl.ds((rows - 1) * 8, 8)], dst_ref=rim_recv.at[step],
            send_sem=edge_send_sem.at[step, 1], recv_sem=edge_recv_sem.at[step, 1],
            device_id=after, device_id_type=MESH,
        )
        edge.start()

        if step == 0:
            for b in range(5 * tiles):
                low = tile_ids[pl.ds(b, 1), :] & (LANES - 1)
                tile_hot[:, pl.ds(b * LANES, LANES)] = (sub == low).astype(F32).astype(BF16)
            for g in range(group):
                for half in range(halves):
                    low = send_in[0, pl.ds(g, 1), pl.ds(half * LANES, LANES)] & (LANES - 1)
                    node_hot[:, pl.ds((g * halves + half) * LANES, LANES)] = (
                        (sub == low).astype(F32).astype(BF16)
                    )
            ids = tile_ids[...]
            ids_low, ids_high = ids & (LANES - 1), ids >> 7

        for d in range(1, group):
            group_copy(step, d, False).wait_recv()
        state = [jnp.zeros(ids.shape, F32) for c in range(6)]
        for g in range(group):
            for half in range(halves):
                match = ids_high == g * halves + half
                for c in range(6):
                    row = jnp.broadcast_to(
                        recv_buf[step, g, pl.ds(c * halves + half, 1), :], ids.shape
                    )
                    state[c] = jnp.where(match, lane_take(row, ids_low), state[c])
        centre = [
            0.25 * sum(s[(a + 1) * tiles : (a + 2) * tiles] for a in range(4)) for s in state
        ]
        nodes = [s[:tiles] for s in state]
        node_mix = [STIFFNESS * nodes[k] - DAMPING * nodes[3 + k] for k in range(3)]
        facet_mix = [STIFFNESS * centre[k] - DAMPING * centre[3 + k] for k in range(3)]
        lead = jnp.concatenate(nodes[:3] + [jnp.zeros((16 - 3 * tiles % 16, LANES), F32)], axis=0)
        columns = jnp.transpose(lead)
        ones = jnp.ones((1, LANES), F32)
        blank = jnp.zeros((4, LANES), F32)
        node_force = [[None] * tiles for k in range(3)]
        facet_force = [[None] * tiles for k in range(3)]
        for t in range(tiles):
            live = jnp.where(t < count_in[0], 1.0, 0.0)
            dist = jnp.zeros((LANES, LANES), F32)
            for k in range(3):
                gap = columns[:, k * tiles + t : k * tiles + t + 1] - centre[k][t : t + 1]
                dist += gap * gap
            weight = mask_in[t].astype(F32) * (live * jnp.maximum(RADIUS_SQ - dist, 0.0))
            w1, w2 = two_parts(weight)
            a1, a2 = two_parts(jnp.concatenate([m[t : t + 1] for m in node_mix] + [ones, blank], axis=0))
            b1, b2 = two_parts(jnp.concatenate([m[t : t + 1] for m in facet_mix] + [ones, blank], axis=0))
            left_a = jnp.concatenate([a1, a2], axis=0)
            left_b = jnp.concatenate([b1, b2], axis=0)
            to_facet = nn_dot(
                jnp.concatenate([left_a, left_a], axis=1), jnp.concatenate([w1, w2], axis=0)
            )
            to_node = nt_dot(
                jnp.concatenate([left_b, left_b], axis=1), jnp.concatenate([w1, w2], axis=1)
            )
            to_facet = to_facet[:8] + to_facet[8:]
            to_node = to_node[:8] + to_node[8:]
            for k in range(3):
                node_force[k][t] = node_mix[k][t : t + 1] * to_node[3:4] - to_node[k : k + 1]
                facet_force[k][t] = -0.25 * (
                    to_facet[k : k + 1] - to_facet[3:4] * facet_mix[k][t : t + 1]
                )
        spans = halves * group
        high_iota = lax.broadcasted_iota(jnp.int32, (spans, LANES), 0)
        for b in range(5 * tiles):
            high = ids_high[b : b + 1]
            match = high_iota == (high % halves) * group + high // halves
            for k in range(3):
                row = node_force[k][b] if b < tiles else facet_force[k][b % tiles]
                chosen = jnp.where(match, jnp.broadcast_to(row, match.shape), 0.0)
                p1, p2 = two_parts(chosen)
                cols = pl.ds(b * LANES, LANES)
                tile_lhs[pl.ds(k * spans, spans), cols] = p1
                tile_lhs[pl.ds((3 + k) * spans, spans), cols] = p2
        slots = nt_dot(tile_lhs[...], tile_hot[...])
        slots = slots[: 3 * spans] + slots[3 * spans :]
        for r in range(3 * halves):
            back_buf[step, :, r, :] = slots[r * group : (r + 1) * group]
        for d in range(1, group):
            group_copy(step, d, True).start()
        answer_buf[step, my_place] = back_buf[step, my_place]
        edge.wait_recv()
        internal = []
        for k in range(3):
            near = rim_send[step, pl.ds(k * 2, rows, stride=8), :]
            far = rim_send[step, pl.ds(k * 2 + 1, rows - 1, stride=8), :]
            edge_row = rim_recv[step, pl.ds(k * 2 + 1, 1), :]
            internal.append(near + jnp.concatenate([edge_row, far], axis=0))
        for d in range(1, group):
            group_copy(step, d, True).wait_recv()
        row_iota = lax.broadcasted_iota(jnp.int32, (rows, LANES), 0)
        for g in range(group):
            for half in range(halves):
                high = send_in[0, pl.ds(g, 1), pl.ds(half * LANES, LANES)] >> 7
                match = row_iota == high
                chosen = jnp.concatenate([
                    jnp.where(
                        match,
                        jnp.broadcast_to(answer_buf[step, g, pl.ds(k * halves + half, 1), :], match.shape),
                        0.0,
                    )
                    for k in range(3)
                ], axis=0)
                first = chosen.astype(BF16).astype(F32)
                both = jnp.concatenate([first, chosen - first], axis=0).astype(BF16)
                node_lhs[:, pl.ds((g * halves + half) * LANES, LANES)] = both
        contact = nt_dot(node_lhs[...], node_hot[...])
        contact = contact[: 3 * rows] + contact[3 * rows :]
        for k in range(3):
            fresh = velocity_rows(k) + TIME_STEP * (
                internal[k] + contact[k * rows : (k + 1) * rows]
            ) / mass
            vel[pl.ds(k * 2 * rows, rows), :] = fresh
            pos[pl.ds(k * rows, rows), :] = pos[pl.ds(k * rows, rows), :] + TIME_STEP * fresh
        if step + 1 < STEPS:
            fill_ghosts(step + 1)
            fill_slots(step + 1)

    for i in range(rows):
        cols = pl.ds(i * LANES, LANES)
        coords_out[:, cols] = pos[pl.ds(i, 3, stride=rows), :]
        velocity_out[:, cols] = vel[pl.ds(i, 3, stride=2 * rows), :]
        stress_out[:, cols] = stress[pl.ds(i, 3, stride=rows), :]
    for step in range(STEPS):
        edge_copy(step, 0).wait_send()
        pltpu.make_async_remote_copy(
            src_ref=rim_send.at[step, pl.ds((rows - 1) * 8, 8)], dst_ref=rim_recv.at[step],
            send_sem=edge_send_sem.at[step, 1], recv_sem=edge_recv_sem.at[step, 1],
            device_id=after, device_id_type=MESH,
        ).wait_send()
        for d in range(1, group):
            group_copy(step, d, False).wait_send()
            group_copy(step, d, True).wait_send()


def per_device(
    sizes, coords, velocity, node_mass, corner_nodes, shape_grad, frame_angles, volume, stress,
    send_nodes, tile_count, tile_nodes, tile_facets, pair_mask,
):
    count = coords.shape[1]
    rows = count // LANES
    group = sizes[1] * sizes[2]
    cap = send_nodes.shape[2]
    tiles = tile_nodes.shape[0]
    spans = group * cap // LANES
    vmem = pl.BlockSpec(memory_space=pltpu.VMEM)
    smem = pl.BlockSpec(memory_space=pltpu.SMEM)
    state = jax.ShapeDtypeStruct((3, count), F32)
    dma = pltpu.SemaphoreType.DMA
    return pl.pallas_call(
        functools.partial(kernel, sizes),
        out_shape=(state, state, state),
        in_specs=[vmem] * 9 + [smem] + [vmem] * 3,
        out_specs=(vmem, vmem, vmem),
        scratch_shapes=[
            pltpu.VMEM((3 * rows, LANES), F32),
            pltpu.VMEM((6 * rows, LANES), F32),
            pltpu.VMEM((4 * rows, LANES), jnp.int32),
            pltpu.VMEM((8 * rows, LANES), F32),
            pltpu.VMEM((3 * rows, LANES), F32),
            pltpu.VMEM((2 * rows, LANES), F32),
            pltpu.VMEM((8, LANES), jnp.int32),
            pltpu.VMEM((-(-5 * tiles // 8) * 8, LANES), jnp.int32),
            pltpu.VMEM((rows, LANES, 4 * LANES), BF16),
            pltpu.VMEM((LANES, 5 * tiles * LANES), BF16),
            pltpu.VMEM((LANES, group * cap), BF16),
            pltpu.VMEM((4, 16 * rows, LANES), F32),
            pltpu.VMEM((6 * spans, 5 * tiles * LANES), BF16),
            pltpu.VMEM((6 * rows, group * cap), BF16),
            pltpu.VMEM((STEPS, group, OUT_ROWS, LANES), F32),
            pltpu.VMEM((STEPS, group, OUT_ROWS, LANES), F32),
            pltpu.VMEM((STEPS, group, BACK_ROWS, LANES), F32),
            pltpu.VMEM((STEPS, group, BACK_ROWS, LANES), F32),
            pltpu.VMEM((STEPS, 3, LANES), F32),
            pltpu.VMEM((STEPS, 3, LANES), F32),
            pltpu.VMEM((STEPS, 8 * rows, LANES), F32),
            pltpu.VMEM((STEPS, 8, LANES), F32),
            dma((STEPS, group - 1)),
            dma((STEPS, group - 1)),
            dma((STEPS, group - 1)),
            dma((STEPS, group - 1)),
            dma((STEPS, 2)),
            dma((STEPS, 2)),
        ],
        compiler_params=pltpu.CompilerParams(collective_id=0, has_side_effects=True),
    )(
        coords, velocity, node_mass.reshape(rows, LANES), corner_nodes, shape_grad, frame_angles,
        volume.reshape(rows, LANES), stress, send_nodes, tile_count, tile_nodes, tile_facets, pair_mask,
    )


def solution(mesh):
    axes = ("len", "wid", "dep")
    flat, wide = P(axes), P(None, axes)
    sizes = tuple(mesh.shape[name] for name in axes)
    return jax.shard_map(
        functools.partial(per_device, sizes),
        mesh=mesh,
        in_specs=(
            wide, wide, flat, wide, wide, wide, flat, wide,
            P(axes, None, None), flat, P(axes, None), P(None, axes, None), P(axes, None, None),
        ),
        out_specs=(wide, wide, wide),
        check_vma=False,
    )
```

```python
import functools

import jax
import jax.numpy as jnp
from jax import lax
from jax.experimental import pallas as pl
from jax.experimental.pallas import tpu as pltpu
from jax.sharding import PartitionSpec as P

STEPS = 2
TIME_STEP = 0.1
YOUNG_MOD = 1.0
POISSON = 0.3
HOURGLASS = 0.1
RADIUS_SQ = 1.0
STIFFNESS = 0.1
DAMPING = 0.05

LANES = 128
MESH = pl.DeviceIdType.MESH
F32 = jnp.float32
BF16 = jnp.bfloat16


def two_parts(values):
    first = values.astype(BF16)
    return first, (values - first.astype(F32)).astype(BF16)


def lane_take(table, low):
    return jnp.take_along_axis(table, low, axis=1, mode="promise_in_bounds")


def nt_dot(left, right):
    return lax.dot_general(left, right, (((1,), (1,)), ((), ())), preferred_element_type=F32)


def nn_dot(left, right):
    return lax.dot_general(left, right, (((1,), (0,)), ((), ())), preferred_element_type=F32)


def kernel(
    sizes,
    coords_hbm, velocity_hbm, mass_hbm, corner_hbm, grad_hbm, angles_hbm, volume_hbm, stress_hbm,
    send_hbm, count_in, nodes_hbm, facets_hbm, mask_hbm,
    coords_out, velocity_out, stress_out,
    coords_in, velocity_in, mass_in, corner_in, grad_in, angles_in, volume_in, stress_in,
    send_in, nodes_in, facets_in, mask_in, in_sem,
    pos, vel, corner, grad, stress, angle, slot_high, tile_ids, win_hot, tile_hot, node_hot,
    win_rows, tile_lhs, node_lhs,
    send_buf, recv_buf, again_buf, fresh_buf, back_buf, answer_buf, ghost_send, ghost_recv, rim_send, rim_recv,
    out_send_sem, out_recv_sem, back_send_sem, back_recv_sem, edge_send_sem, edge_recv_sem,
):
    n_len, n_wid, n_dep = sizes
    group = n_wid * n_dep
    devices = n_len * group
    rows = coords_in.shape[1] // LANES
    order = sorted(range(1, group), key=lambda d: -min(d, group - d))
    halves = send_in.shape[2] // LANES
    tiles = nodes_in.shape[0]
    my_len = lax.axis_index("len")
    my_place = lax.axis_index("wid") * n_dep + lax.axis_index("dep")
    my_id = my_len * group + my_place

    def by_id(p):
        return (p // group, (p % group) // n_dep, p % n_dep)

    def partner(d):
        g = lax.rem(my_place + d, group)
        return g, (my_len, g // n_dep, lax.rem(g, n_dep))

    before = by_id(lax.rem(my_id + devices - 1, devices))
    after = by_id(lax.rem(my_id + 1, devices))

    loads = [
        pltpu.make_async_copy(src, dst, in_sem.at[n])
        for n, (src, dst) in enumerate((
            (coords_hbm, coords_in), (velocity_hbm, velocity_in), (send_hbm, send_in),
            (corner_hbm, corner_in), (stress_hbm, stress_in), (grad_hbm, grad_in),
            (angles_hbm, angles_in), (mass_hbm, mass_in), (volume_hbm, volume_in),
            (nodes_hbm, nodes_in), (facets_hbm, facets_in), (mask_hbm, mask_in),
        ))
    ]
    barrier = pltpu.get_barrier_semaphore()
    for d in order:
        pl.semaphore_signal(barrier, inc=1, device_id=partner(d)[1], device_id_type=MESH)
    pl.semaphore_signal(barrier, inc=1, device_id=before, device_id_type=MESH)
    pl.semaphore_signal(barrier, inc=1, device_id=after, device_id_type=MESH)

    for load in loads:
        load.start()
    for load in loads[:3]:
        load.wait()
    for i in range(rows):
        cols = pl.ds(i * LANES, LANES)
        pos[pl.ds(i, 3, stride=rows), :] = coords_in[:, cols]
        for k in range(3):
            vel[pl.ds(k * 2 * rows + i, 1), :] = velocity_in[pl.ds(k, 1), cols]

    def velocity_rows(k):
        return vel[pl.ds(k * 2 * rows, rows), :]

    def fill_ghosts(step):
        for k in range(3):
            ghost_send[step, pl.ds(k, 1), :] = vel[pl.ds(k * 2 * rows, 1), :]

    def fill_slots(step):
        tables = [velocity_rows(k) for k in range(3)]
        if step == 0:
            tables += [pos[pl.ds(k * rows, rows), :] for k in range(3)]
        for half in range(halves):
            ids = send_in[0, :, pl.ds(half * LANES, LANES)]
            low, high = ids & (LANES - 1), ids >> 7
            if step == 0:
                slot_high[:, half, :] = high
            for c, table in enumerate(tables):
                found = jnp.zeros(ids.shape, F32)
                for h in range(rows):
                    row = jnp.broadcast_to(table[h : h + 1], ids.shape)
                    found = jnp.where(high == h, lane_take(row, low), found)
                if step == 0:
                    send_buf[:, c * halves + half, :] = found
                else:
                    again_buf[step - 1, :, c * halves + half, :] = found

    fill_ghosts(0)
    fill_slots(0)
    for load in loads[3:]:
        load.wait()
    for i in range(rows):
        cols = pl.ds(i * LANES, LANES)
        stress[pl.ds(i, 3, stride=rows), :] = stress_in[:, cols]
        corner[pl.ds(i, 4, stride=rows), :] = corner_in[:, cols]
        grad[pl.ds(i, 8, stride=rows), :] = grad_in[:, cols]
        angle[pl.ds(i, 2, stride=rows), :] = angles_in[:, cols]
    tile_rows = tile_ids.shape[0]
    tile_ids[...] = jnp.zeros_like(tile_ids)
    tile_ids[pl.ds(0, tiles), :] = nodes_in[...]
    for a in range(4):
        tile_ids[pl.ds((a + 1) * tiles, tiles), :] = facets_in[a]

    def edge_copy(step, which):
        src, dst, target = ((ghost_send, ghost_recv, before), (rim_send, rim_recv, after))[which]
        return pltpu.make_async_remote_copy(
            src_ref=src.at[step], dst_ref=dst.at[step],
            send_sem=edge_send_sem.at[step, which], recv_sem=edge_recv_sem.at[step, which],
            device_id=target, device_id_type=MESH,
        )

    def group_copy(step, d, back):
        g, target = partner(d)
        if back:
            src, dst, ss, rs = back_buf.at[step], answer_buf.at[step], back_send_sem, back_recv_sem
        elif step == 0:
            src, dst, ss, rs = send_buf, recv_buf, out_send_sem, out_recv_sem
        else:
            src, dst, ss, rs = again_buf.at[step - 1], fresh_buf.at[step - 1], out_send_sem, out_recv_sem
        return pltpu.make_async_remote_copy(
            src_ref=src.at[g], dst_ref=dst.at[my_place],
            send_sem=ss.at[step, d - 1], recv_sem=rs.at[step, d - 1],
            device_id=target, device_id_type=MESH,
        )

    pl.semaphore_wait(barrier, group + 1)

    sub = lax.broadcasted_iota(jnp.int32, (LANES, LANES), 0)
    for step in range(STEPS):
        edge_copy(step, 0).start()
        for d in order:
            group_copy(step, d, False).start()
        if step == 0:
            recv_buf[my_place] = send_buf[my_place]
        else:
            fresh_buf[step - 1, my_place] = again_buf[step - 1, my_place]

        if step == 0:
            first_row = lax.broadcasted_iota(jnp.int32, (rows, LANES), 0) * LANES
            corner_low, corner_far = [], []
            for a in range(4):
                local = corner[pl.ds(a * rows, rows), :] - first_row
                corner_low.append(local & (LANES - 1))
                corner_far.append(local >= LANES)
                for i in range(rows):
                    hot = (sub == corner_low[a][i : i + 1]).astype(F32).astype(BF16)
                    win_hot[i, :, pl.ds(a * LANES, LANES)] = hot
            polar, azim = angle[pl.ds(0, rows), :], angle[pl.ds(rows, rows), :]
            cos_p, sin_p, cos_a, sin_a = jnp.cos(polar), jnp.sin(polar), jnp.cos(azim), jnp.sin(azim)
            one = (cos_p * cos_a, cos_p * sin_a, -sin_p)
            two = (-sin_a, cos_a)
            volume = volume_in[...]
            mass = mass_in[...]
            gx = [grad[pl.ds(a * rows, rows), :] for a in range(4)]
            gy = [grad[pl.ds((4 + a) * rows, rows), :] for a in range(4)]

        edge_copy(step, 0).wait_recv()
        for k in range(3):
            vel[pl.ds(k * 2 * rows + rows, 1), :] = ghost_recv[step, pl.ds(k, 1), :]
        corner_vel = []
        for k in range(3):
            near = velocity_rows(k)
            far = vel[pl.ds(k * 2 * rows + 1, rows), :]
            corner_vel.append([
                jnp.where(corner_far[a], lane_take(far, corner_low[a]), lane_take(near, corner_low[a]))
                for a in range(4)
            ])
        xx = yy = xy = jnp.zeros((rows, LANES), F32)
        for a in range(4):
            u = sum(one[k] * corner_vel[k][a] for k in range(3))
            w = sum(two[k] * corner_vel[k][a] for k in range(2))
            xx += gx[a] * u
            yy += gy[a] * w
            xy += gy[a] * u + gx[a] * w
        factor = TIME_STEP * YOUNG_MOD / (1.0 - POISSON * POISSON)
        sxx = stress[pl.ds(0, rows), :] + factor * (xx + POISSON * yy)
        syy = stress[pl.ds(rows, rows), :] + factor * (POISSON * xx + yy)
        sxy = stress[pl.ds(2 * rows, rows), :] + factor * 0.5 * (1.0 - POISSON) * xy
        stress[pl.ds(0, rows), :] = sxx
        stress[pl.ds(rows, rows), :] = syy
        stress[pl.ds(2 * rows, rows), :] = sxy
        hour = [
            HOURGLASS * volume
            * (corner_vel[k][0] - corner_vel[k][1] + corner_vel[k][2] - corner_vel[k][3])
            for k in range(3)
        ]
        for a in range(4):
            f1 = -volume * (gx[a] * sxx + gy[a] * sxy)
            f2 = -volume * (gy[a] * syy + gx[a] * sxy)
            for k in range(3):
                force = one[k] * f1 - (1.0 if a % 2 == 0 else -1.0) * hour[k]
                if k < 2:
                    force += two[k] * f2
                first = force.astype(BF16).astype(F32)
                for part, value in enumerate((first, force - first)):
                    for side in range(2):
                        keep = corner_far[a] if side else jnp.logical_not(corner_far[a])
                        win_rows[a, pl.ds(part * 8 + k * 2 + side, rows, stride=16), :] = jnp.where(
                            keep, value, 0.0
                        )
        for i in range(rows):
            left = jnp.concatenate(
                [win_rows[a, pl.ds(i * 16, 16), :].astype(BF16) for a in range(4)], axis=1
            )
            summed = nt_dot(left, win_hot[i])
            rim_send[step, pl.ds(i * 8, 8), :] = summed[:8] + summed[8:]
        edge = pltpu.make_async_remote_copy(
            src_ref=rim_send.at[step, pl.ds((rows - 1) * 8, 8)], dst_ref=rim_recv.at[step],
            send_sem=edge_send_sem.at[step, 1], recv_sem=edge_recv_sem.at[step, 1],
            device_id=after, device_id_type=MESH,
        )
        edge.start()

        if step == 0:
            for b in range(5 * tiles):
                low = tile_ids[pl.ds(b, 1), :] & (LANES - 1)
                tile_hot[:, pl.ds(b * LANES, LANES)] = (sub == low).astype(F32).astype(BF16)
            for g in range(group):
                for half in range(halves):
                    low = send_in[0, pl.ds(g, 1), pl.ds(half * LANES, LANES)] & (LANES - 1)
                    node_hot[:, pl.ds((g * halves + half) * LANES, LANES)] = (
                        (sub == low).astype(F32).astype(BF16)
                    )
            ids = tile_ids[...]
            ids_low, ids_high = ids & (LANES - 1), ids >> 7

        landed = recv_buf if step == 0 else fresh_buf.at[step - 1]
        found = [jnp.zeros(ids.shape, F32) for c in range(6 if step == 0 else 3)]
        for d in [0] + order[::-1]:
            if d:
                group_copy(step, d, False).wait_recv()
            g = lax.rem(my_place + group - d, group)
            for half in range(halves):
                match = ids_high == g * halves + half
                for c in range(len(found)):
                    row = jnp.broadcast_to(landed[g, pl.ds(c * halves + half, 1), :], ids.shape)
                    found[c] = jnp.where(match, lane_take(row, ids_low), found[c])
        if step == 0:
            slot_pos = found[3:]
        else:
            slot_pos = [slot_pos[k] + TIME_STEP * found[k] for k in range(3)]
        state = slot_pos + found[:3]
        centre = [
            0.25 * sum(s[(a + 1) * tiles : (a + 2) * tiles] for a in range(4)) for s in state
        ]
        nodes = [s[:tiles] for s in state]
        node_mix = [STIFFNESS * nodes[k] - DAMPING * nodes[3 + k] for k in range(3)]
        facet_mix = [STIFFNESS * centre[k] - DAMPING * centre[3 + k] for k in range(3)]
        lead = jnp.concatenate(nodes[:3] + [jnp.zeros((16 - 3 * tiles % 16, LANES), F32)], axis=0)
        columns = jnp.transpose(lead)
        ones = jnp.ones((1, LANES), F32)
        blank = jnp.zeros((4, LANES), F32)
        node_force = [[None] * tiles for k in range(3)]
        facet_force = [[None] * tiles for k in range(3)]
        for t in range(tiles):
            live = jnp.where(t < count_in[0], 1.0, 0.0)
            dist = jnp.zeros((LANES, LANES), F32)
            for k in range(3):
                gap = columns[:, k * tiles + t : k * tiles + t + 1] - centre[k][t : t + 1]
                dist += gap * gap
            weight = mask_in[t].astype(F32) * (live * jnp.maximum(RADIUS_SQ - dist, 0.0))
            w1, w2 = two_parts(weight)
            a1, a2 = two_parts(jnp.concatenate([m[t : t + 1] for m in node_mix] + [ones, blank], axis=0))
            b1, b2 = two_parts(jnp.concatenate([m[t : t + 1] for m in facet_mix] + [ones, blank], axis=0))
            left_a = jnp.concatenate([a1, a2], axis=0)
            left_b = jnp.concatenate([b1, b2], axis=0)
            to_facet = nn_dot(
                jnp.concatenate([left_a, left_a], axis=1), jnp.concatenate([w1, w2], axis=0)
            )
            to_node = nt_dot(
                jnp.concatenate([left_b, left_b], axis=1), jnp.concatenate([w1, w2], axis=1)
            )
            to_facet = to_facet[:8] + to_facet[8:]
            to_node = to_node[:8] + to_node[8:]
            for k in range(3):
                node_force[k][t] = node_mix[k][t : t + 1] * to_node[3:4] - to_node[k : k + 1]
                facet_force[k][t] = -0.25 * (
                    to_facet[k : k + 1] - to_facet[3:4] * facet_mix[k][t : t + 1]
                )
        spans = halves * group
        high_iota = lax.broadcasted_iota(jnp.int32, (spans, LANES), 0)
        for b in range(5 * tiles):
            high = ids_high[b : b + 1]
            match = high_iota == (high % halves) * group + high // halves
            for k in range(3):
                row = node_force[k][b] if b < tiles else facet_force[k][b % tiles]
                chosen = jnp.where(match, jnp.broadcast_to(row, match.shape), 0.0)
                p1, p2 = two_parts(chosen)
                cols = pl.ds(b * LANES, LANES)
                tile_lhs[pl.ds(k * spans, spans), cols] = p1
                tile_lhs[pl.ds((3 + k) * spans, spans), cols] = p2
        slots = nt_dot(tile_lhs[...], tile_hot[...])
        slots = slots[: 3 * spans] + slots[3 * spans :]
        for r in range(3 * halves):
            back_buf[step, :, r, :] = slots[r * group : (r + 1) * group]
        for d in order:
            group_copy(step, d, True).start()
        answer_buf[step, my_place] = back_buf[step, my_place]
        edge.wait_recv()
        internal = []
        for k in range(3):
            near = rim_send[step, pl.ds(k * 2, rows, stride=8), :]
            far = rim_send[step, pl.ds(k * 2 + 1, rows - 1, stride=8), :]
            edge_row = rim_recv[step, pl.ds(k * 2 + 1, 1), :]
            internal.append(near + jnp.concatenate([edge_row, far], axis=0))
        row_iota = lax.broadcasted_iota(jnp.int32, (rows, LANES), 0)
        for d in [0] + order[::-1]:
            if d:
                group_copy(step, d, True).wait_recv()
            g = lax.rem(my_place + group - d, group)
            for half in range(halves):
                high = slot_high[g, pl.ds(half, 1), :]
                match = row_iota == high
                chosen = jnp.concatenate([
                    jnp.where(
                        match,
                        jnp.broadcast_to(answer_buf[step, g, pl.ds(k * halves + half, 1), :], match.shape),
                        0.0,
                    )
                    for k in range(3)
                ], axis=0)
                first = chosen.astype(BF16).astype(F32)
                both = jnp.concatenate([first, chosen - first], axis=0).astype(BF16)
                start = pl.multiple_of((g * halves + half) * LANES, LANES)
                node_lhs[:, pl.ds(start, LANES)] = both
        contact = nt_dot(node_lhs[...], node_hot[...])
        contact = contact[: 3 * rows] + contact[3 * rows :]
        for k in range(3):
            fresh = velocity_rows(k) + TIME_STEP * (
                internal[k] + contact[k * rows : (k + 1) * rows]
            ) / mass
            vel[pl.ds(k * 2 * rows, rows), :] = fresh
            pos[pl.ds(k * rows, rows), :] = pos[pl.ds(k * rows, rows), :] + TIME_STEP * fresh
        if step + 1 < STEPS:
            fill_ghosts(step + 1)
            fill_slots(step + 1)

    coords_out[...] = pos[...]
    for k in range(3):
        velocity_out[pl.ds(k * rows, rows), :] = velocity_rows(k)
    stress_out[...] = stress[...]
    for step in range(STEPS):
        edge_copy(step, 0).wait_send()
        pltpu.make_async_remote_copy(
            src_ref=rim_send.at[step, pl.ds((rows - 1) * 8, 8)], dst_ref=rim_recv.at[step],
            send_sem=edge_send_sem.at[step, 1], recv_sem=edge_recv_sem.at[step, 1],
            device_id=after, device_id_type=MESH,
        ).wait_send()
        for d in range(1, group):
            group_copy(step, d, False).wait_send()
            group_copy(step, d, True).wait_send()


def arrange(coords_rows, velocity_rows, stress_rows, coords_out, velocity_out, stress_out):
    rows = coords_rows.shape[0] // 3
    pairs = ((coords_rows, coords_out), (velocity_rows, velocity_out), (stress_rows, stress_out))
    for source, target in pairs:
        for i in range(rows):
            target[:, pl.ds(i * LANES, LANES)] = source[pl.ds(i, 3, stride=rows), :]


def per_device(
    sizes, coords, velocity, node_mass, corner_nodes, shape_grad, frame_angles, volume, stress,
    send_nodes, tile_count, tile_nodes, tile_facets, pair_mask,
):
    count = coords.shape[1]
    rows = count // LANES
    group = sizes[1] * sizes[2]
    cap = send_nodes.shape[2]
    tiles = tile_nodes.shape[0]
    spans = group * cap // LANES
    vmem = pl.BlockSpec(memory_space=pltpu.VMEM)
    smem = pl.BlockSpec(memory_space=pltpu.SMEM)
    state = jax.ShapeDtypeStruct((3, count), F32)
    packed = jax.ShapeDtypeStruct((3 * rows, LANES), F32)
    hbm = pl.BlockSpec(memory_space=pl.ANY)
    halves = cap // LANES
    arrays = (
        coords, velocity, node_mass.reshape(rows, LANES), corner_nodes, shape_grad, frame_angles,
        volume.reshape(rows, LANES), stress, send_nodes, tile_nodes, tile_facets, pair_mask,
    )
    dma = pltpu.SemaphoreType.DMA
    finals = pl.pallas_call(
        functools.partial(kernel, sizes),
        out_shape=(packed, packed, packed),
        in_specs=[hbm] * 9 + [smem] + [hbm] * 3,
        out_specs=(vmem, vmem, vmem),
        scratch_shapes=[pltpu.VMEM(a.shape, a.dtype) for a in arrays] + [
            dma((len(arrays),)),
            pltpu.VMEM((3 * rows, LANES), F32),
            pltpu.VMEM((6 * rows, LANES), F32),
            pltpu.VMEM((4 * rows, LANES), jnp.int32),
            pltpu.VMEM((8 * rows, LANES), F32),
            pltpu.VMEM((3 * rows, LANES), F32),
            pltpu.VMEM((2 * rows, LANES), F32),
            pltpu.VMEM((group, halves, LANES), jnp.int32),
            pltpu.VMEM((-(-5 * tiles // 8) * 8, LANES), jnp.int32),
            pltpu.VMEM((rows, LANES, 4 * LANES), BF16),
            pltpu.VMEM((LANES, 5 * tiles * LANES), BF16),
            pltpu.VMEM((LANES, group * cap), BF16),
            pltpu.VMEM((4, 16 * rows, LANES), F32),
            pltpu.VMEM((6 * spans, 5 * tiles * LANES), BF16),
            pltpu.VMEM((6 * rows, group * cap), BF16),
            pltpu.VMEM((group, 6 * halves, LANES), F32),
            pltpu.VMEM((group, 6 * halves, LANES), F32),
            pltpu.VMEM((STEPS - 1, group, 3 * halves, LANES), F32),
            pltpu.VMEM((STEPS - 1, group, 3 * halves, LANES), F32),
            pltpu.VMEM((STEPS, group, 3 * halves, LANES), F32),
            pltpu.VMEM((STEPS, group, 3 * halves, LANES), F32),
            pltpu.VMEM((STEPS, 3, LANES), F32),
            pltpu.VMEM((STEPS, 3, LANES), F32),
            pltpu.VMEM((STEPS, 8 * rows, LANES), F32),
            pltpu.VMEM((STEPS, 8, LANES), F32),
            dma((STEPS, group - 1)),
            dma((STEPS, group - 1)),
            dma((STEPS, group - 1)),
            dma((STEPS, group - 1)),
            dma((STEPS, 2)),
            dma((STEPS, 2)),
        ],
        compiler_params=pltpu.CompilerParams(collective_id=0, has_side_effects=True),
    )(*arrays[:9], tile_count, *arrays[9:])
    return pl.pallas_call(
        arrange,
        out_shape=(state, state, state),
        in_specs=[vmem] * 3,
        out_specs=(vmem, vmem, vmem),
    )(*finals)


def solution(mesh):
    axes = ("len", "wid", "dep")
    flat, wide = P(axes), P(None, axes)
    sizes = tuple(mesh.shape[name] for name in axes)
    return jax.shard_map(
        functools.partial(per_device, sizes),
        mesh=mesh,
        in_specs=(
            wide, wide, flat, wide, wide, wide, flat, wide,
            P(axes, None, None), flat, P(axes, None), P(None, axes, None), P(axes, None, None),
        ),
        out_specs=(wide, wide, wide),
        check_vma=False,
    )
```

```python
import functools

import jax
import jax.numpy as jnp
from jax import lax
from jax.experimental import pallas as pl
from jax.experimental.pallas import tpu as pltpu
from jax.sharding import PartitionSpec as P

STEPS = 2
TIME_STEP = 0.1
YOUNG_MOD = 1.0
POISSON = 0.3
HOURGLASS = 0.1
RADIUS_SQ = 1.0
STIFFNESS = 0.1
DAMPING = 0.05

LANES = 128
MESH = pl.DeviceIdType.MESH
F32 = jnp.float32
BF16 = jnp.bfloat16


def two_parts(values):
    first = values.astype(BF16)
    return first, (values - first.astype(F32)).astype(BF16)


def lane_take(table, low):
    return jnp.take_along_axis(table, low, axis=1, mode="promise_in_bounds")


def nt_dot(left, right):
    return lax.dot_general(left, right, (((1,), (1,)), ((), ())), preferred_element_type=F32)


def nn_dot(left, right):
    return lax.dot_general(left, right, (((1,), (0,)), ((), ())), preferred_element_type=F32)


def kernel(
    sizes,
    coords_hbm, velocity_hbm, mass_hbm, corner_hbm, grad_hbm, angles_hbm, volume_hbm, stress_hbm,
    send_hbm, count_in, nodes_hbm, facets_hbm, mask_hbm,
    coords_out, velocity_out, stress_out,
    coords_in, velocity_in, mass_in, corner_in, grad_in, angles_in, volume_in, stress_in,
    send_in, nodes_in, facets_in, mask_in, in_sem,
    pos, vel, corner, grad, stress, angle, slot_high, tile_ids, win_hot, tile_hot, node_hot,
    win_rows, tile_lhs, node_lhs,
    send_buf, recv_buf, again_buf, fresh_buf, back_buf, answer_buf, ghost_send, ghost_recv, rim_send, rim_recv,
    out_send_sem, out_recv_sem, back_send_sem, back_recv_sem, edge_send_sem, edge_recv_sem,
):
    n_len, n_wid, n_dep = sizes
    group = n_wid * n_dep
    devices = n_len * group
    rows = coords_in.shape[1] // LANES
    order = sorted(range(1, group), key=lambda d: -min(d, group - d))
    halves = send_in.shape[2] // LANES
    tiles = nodes_in.shape[0]
    my_len = lax.axis_index("len")
    my_place = lax.axis_index("wid") * n_dep + lax.axis_index("dep")
    my_id = my_len * group + my_place

    def by_id(p):
        return (p // group, (p % group) // n_dep, p % n_dep)

    def partner(d):
        g = lax.rem(my_place + d, group)
        return g, (my_len, g // n_dep, lax.rem(g, n_dep))

    before = by_id(lax.rem(my_id + devices - 1, devices))
    after = by_id(lax.rem(my_id + 1, devices))

    loads = [
        pltpu.make_async_copy(src, dst, in_sem.at[n])
        for n, (src, dst) in enumerate((
            (coords_hbm, coords_in), (velocity_hbm, velocity_in), (send_hbm, send_in),
            (corner_hbm, corner_in), (stress_hbm, stress_in), (grad_hbm, grad_in),
            (angles_hbm, angles_in), (mass_hbm, mass_in), (volume_hbm, volume_in),
            (nodes_hbm, nodes_in), (facets_hbm, facets_in), (mask_hbm, mask_in),
        ))
    ]
    barrier = pltpu.get_barrier_semaphore()
    for d in order:
        pl.semaphore_signal(barrier, inc=1, device_id=partner(d)[1], device_id_type=MESH)
    pl.semaphore_signal(barrier, inc=1, device_id=before, device_id_type=MESH)
    pl.semaphore_signal(barrier, inc=1, device_id=after, device_id_type=MESH)

    for load in loads:
        load.start()
    for load in loads[:3]:
        load.wait()
    for i in range(rows):
        cols = pl.ds(i * LANES, LANES)
        pos[pl.ds(i, 3, stride=rows), :] = coords_in[:, cols]
        for k in range(3):
            vel[pl.ds(k * 2 * rows + i, 1), :] = velocity_in[pl.ds(k, 1), cols]

    def velocity_rows(k):
        return vel[pl.ds(k * 2 * rows, rows), :]

    def fill_ghosts(step):
        for k in range(3):
            ghost_send[step, pl.ds(k, 1), :] = vel[pl.ds(k * 2 * rows, 1), :]

    def fill_slots(step):
        tables = [velocity_rows(k) for k in range(3)]
        if step == 0:
            tables += [pos[pl.ds(k * rows, rows), :] for k in range(3)]
        for half in range(halves):
            ids = send_in[0, :, pl.ds(half * LANES, LANES)]
            low, high = ids & (LANES - 1), ids >> 7
            if step == 0:
                slot_high[:, half, :] = high
            for c, table in enumerate(tables):
                found = jnp.zeros(ids.shape, F32)
                for h in range(rows):
                    row = jnp.broadcast_to(table[h : h + 1], ids.shape)
                    found = jnp.where(high == h, lane_take(row, low), found)
                if step == 0:
                    send_buf[:, c * halves + half, :] = found
                else:
                    again_buf[step - 1, :, c * halves + half, :] = found

    fill_ghosts(0)
    fill_slots(0)
    for load in loads[3:]:
        load.wait()
    for i in range(rows):
        cols = pl.ds(i * LANES, LANES)
        stress[pl.ds(i, 3, stride=rows), :] = stress_in[:, cols]
        corner[pl.ds(i, 4, stride=rows), :] = corner_in[:, cols]
        grad[pl.ds(i, 8, stride=rows), :] = grad_in[:, cols]
        angle[pl.ds(i, 2, stride=rows), :] = angles_in[:, cols]
    tile_rows = tile_ids.shape[0]
    tile_ids[...] = jnp.zeros_like(tile_ids)
    tile_ids[pl.ds(0, tiles), :] = nodes_in[...]
    for a in range(4):
        tile_ids[pl.ds((a + 1) * tiles, tiles), :] = facets_in[a]

    def edge_copy(step, which):
        src, dst, target = ((ghost_send, ghost_recv, before), (rim_send, rim_recv, after))[which]
        return pltpu.make_async_remote_copy(
            src_ref=src.at[step], dst_ref=dst.at[step],
            send_sem=edge_send_sem.at[step, which], recv_sem=edge_recv_sem.at[step, which],
            device_id=target, device_id_type=MESH,
        )

    def group_copy(step, d, back):
        g, target = partner(d)
        if back:
            src, dst, ss, rs = back_buf.at[step], answer_buf.at[step], back_send_sem, back_recv_sem
        elif step == 0:
            src, dst, ss, rs = send_buf, recv_buf, out_send_sem, out_recv_sem
        else:
            src, dst, ss, rs = again_buf.at[step - 1], fresh_buf.at[step - 1], out_send_sem, out_recv_sem
        return pltpu.make_async_remote_copy(
            src_ref=src.at[g], dst_ref=dst.at[my_place],
            send_sem=ss.at[step, d - 1], recv_sem=rs.at[step, d - 1],
            device_id=target, device_id_type=MESH,
        )

    pl.semaphore_wait(barrier, group + 1)

    sub = lax.broadcasted_iota(jnp.int32, (LANES, LANES), 0)
    for step in range(STEPS):
        edge_copy(step, 0).start()
        for d in order:
            group_copy(step, d, False).start()
        if step == 0:
            recv_buf[my_place] = send_buf[my_place]
        else:
            fresh_buf[step - 1, my_place] = again_buf[step - 1, my_place]

        if step == 0:
            first_row = lax.broadcasted_iota(jnp.int32, (rows, LANES), 0) * LANES
            corner_low, corner_far = [], []
            for a in range(4):
                local = corner[pl.ds(a * rows, rows), :] - first_row
                corner_low.append(local & (LANES - 1))
                corner_far.append(local >= LANES)
                for i in range(rows):
                    hot = (sub == corner_low[a][i : i + 1]).astype(F32).astype(BF16)
                    win_hot[i, :, pl.ds(a * LANES, LANES)] = hot
            polar, azim = angle[pl.ds(0, rows), :], angle[pl.ds(rows, rows), :]
            cos_p, sin_p, cos_a, sin_a = jnp.cos(polar), jnp.sin(polar), jnp.cos(azim), jnp.sin(azim)
            one = (cos_p * cos_a, cos_p * sin_a, -sin_p)
            two = (-sin_a, cos_a)
            volume = volume_in[...]
            mass = mass_in[...]
            gx = [grad[pl.ds(a * rows, rows), :] for a in range(4)]
            gy = [grad[pl.ds((4 + a) * rows, rows), :] for a in range(4)]

        edge_copy(step, 0).wait_recv()
        for k in range(3):
            vel[pl.ds(k * 2 * rows + rows, 1), :] = ghost_recv[step, pl.ds(k, 1), :]
        corner_vel = []
        for k in range(3):
            near = velocity_rows(k)
            far = vel[pl.ds(k * 2 * rows + 1, rows), :]
            corner_vel.append([
                jnp.where(corner_far[a], lane_take(far, corner_low[a]), lane_take(near, corner_low[a]))
                for a in range(4)
            ])
        xx = yy = xy = jnp.zeros((rows, LANES), F32)
        for a in range(4):
            u = sum(one[k] * corner_vel[k][a] for k in range(3))
            w = sum(two[k] * corner_vel[k][a] for k in range(2))
            xx += gx[a] * u
            yy += gy[a] * w
            xy += gy[a] * u + gx[a] * w
        factor = TIME_STEP * YOUNG_MOD / (1.0 - POISSON * POISSON)
        sxx = stress[pl.ds(0, rows), :] + factor * (xx + POISSON * yy)
        syy = stress[pl.ds(rows, rows), :] + factor * (POISSON * xx + yy)
        sxy = stress[pl.ds(2 * rows, rows), :] + factor * 0.5 * (1.0 - POISSON) * xy
        stress[pl.ds(0, rows), :] = sxx
        stress[pl.ds(rows, rows), :] = syy
        stress[pl.ds(2 * rows, rows), :] = sxy
        hour = [
            HOURGLASS * volume
            * (corner_vel[k][0] - corner_vel[k][1] + corner_vel[k][2] - corner_vel[k][3])
            for k in range(3)
        ]
        for a in range(4):
            f1 = -volume * (gx[a] * sxx + gy[a] * sxy)
            f2 = -volume * (gy[a] * syy + gx[a] * sxy)
            for k in range(3):
                force = one[k] * f1 - (1.0 if a % 2 == 0 else -1.0) * hour[k]
                if k < 2:
                    force += two[k] * f2
                first = force.astype(BF16).astype(F32)
                for part, value in enumerate((first, force - first)):
                    for side in range(2):
                        keep = corner_far[a] if side else jnp.logical_not(corner_far[a])
                        win_rows[a, pl.ds(part * 8 + k * 2 + side, rows, stride=16), :] = jnp.where(
                            keep, value, 0.0
                        )
        for i in range(rows):
            left = jnp.concatenate(
                [win_rows[a, pl.ds(i * 16, 16), :].astype(BF16) for a in range(4)], axis=1
            )
            summed = nt_dot(left, win_hot[i])
            rim_send[step, pl.ds(i * 8, 8), :] = summed[:8] + summed[8:]
        edge = pltpu.make_async_remote_copy(
            src_ref=rim_send.at[step, pl.ds((rows - 1) * 8, 8)], dst_ref=rim_recv.at[step],
            send_sem=edge_send_sem.at[step, 1], recv_sem=edge_recv_sem.at[step, 1],
            device_id=after, device_id_type=MESH,
        )
        edge.start()

        if step == 0:
            for b in range(5 * tiles):
                low = tile_ids[pl.ds(b, 1), :] & (LANES - 1)
                tile_hot[:, pl.ds(b * LANES, LANES)] = (sub == low).astype(F32).astype(BF16)
            for g in range(group):
                for half in range(halves):
                    low = send_in[0, pl.ds(g, 1), pl.ds(half * LANES, LANES)] & (LANES - 1)
                    node_hot[:, pl.ds((g * halves + half) * LANES, LANES)] = (
                        (sub == low).astype(F32).astype(BF16)
                    )
            ids = tile_ids[...]
            ids_low, ids_high = ids & (LANES - 1), ids >> 7

        landed = recv_buf if step == 0 else fresh_buf.at[step - 1]
        found = [jnp.zeros(ids.shape, F32) for c in range(6 if step == 0 else 3)]
        for d in order[::-1]:
            group_copy(step, d, False).wait_recv()
        for g in range(group):
            for half in range(halves):
                match = ids_high == g * halves + half
                for c in range(len(found)):
                    row = jnp.broadcast_to(landed[g, pl.ds(c * halves + half, 1), :], ids.shape)
                    found[c] = jnp.where(match, lane_take(row, ids_low), found[c])
        if step == 0:
            slot_pos = found[3:]
        else:
            slot_pos = [slot_pos[k] + TIME_STEP * found[k] for k in range(3)]
        state = slot_pos + found[:3]
        centre = [
            0.25 * sum(s[(a + 1) * tiles : (a + 2) * tiles] for a in range(4)) for s in state
        ]
        nodes = [s[:tiles] for s in state]
        node_mix = [STIFFNESS * nodes[k] - DAMPING * nodes[3 + k] for k in range(3)]
        facet_mix = [STIFFNESS * centre[k] - DAMPING * centre[3 + k] for k in range(3)]
        lead = jnp.concatenate(nodes[:3] + [jnp.zeros((16 - 3 * tiles % 16, LANES), F32)], axis=0)
        columns = jnp.transpose(lead)
        ones = jnp.ones((1, LANES), F32)
        blank = jnp.zeros((4, LANES), F32)
        node_force = [[None] * tiles for k in range(3)]
        facet_force = [[None] * tiles for k in range(3)]
        for t in range(tiles):
            live = jnp.where(t < count_in[0], 1.0, 0.0)
            dist = jnp.zeros((LANES, LANES), F32)
            for k in range(3):
                gap = columns[:, k * tiles + t : k * tiles + t + 1] - centre[k][t : t + 1]
                dist += gap * gap
            weight = mask_in[t].astype(F32) * (live * jnp.maximum(RADIUS_SQ - dist, 0.0))
            w1, w2 = two_parts(weight)
            a1, a2 = two_parts(jnp.concatenate([m[t : t + 1] for m in node_mix] + [ones, blank], axis=0))
            b1, b2 = two_parts(jnp.concatenate([m[t : t + 1] for m in facet_mix] + [ones, blank], axis=0))
            left_a = jnp.concatenate([a1, a2], axis=0)
            left_b = jnp.concatenate([b1, b2], axis=0)
            to_facet = nn_dot(
                jnp.concatenate([left_a, left_a], axis=1), jnp.concatenate([w1, w2], axis=0)
            )
            to_node = nt_dot(
                jnp.concatenate([left_b, left_b], axis=1), jnp.concatenate([w1, w2], axis=1)
            )
            to_facet = to_facet[:8] + to_facet[8:]
            to_node = to_node[:8] + to_node[8:]
            for k in range(3):
                node_force[k][t] = node_mix[k][t : t + 1] * to_node[3:4] - to_node[k : k + 1]
                facet_force[k][t] = -0.25 * (
                    to_facet[k : k + 1] - to_facet[3:4] * facet_mix[k][t : t + 1]
                )
        spans = halves * group
        high_iota = lax.broadcasted_iota(jnp.int32, (spans, LANES), 0)
        for b in range(5 * tiles):
            high = ids_high[b : b + 1]
            match = high_iota == (high % halves) * group + high // halves
            for k in range(3):
                row = node_force[k][b] if b < tiles else facet_force[k][b % tiles]
                chosen = jnp.where(match, jnp.broadcast_to(row, match.shape), 0.0)
                p1, p2 = two_parts(chosen)
                cols = pl.ds(b * LANES, LANES)
                tile_lhs[pl.ds(k * spans, spans), cols] = p1
                tile_lhs[pl.ds((3 + k) * spans, spans), cols] = p2
        slots = nt_dot(tile_lhs[...], tile_hot[...])
        slots = slots[: 3 * spans] + slots[3 * spans :]
        for r in range(3 * halves):
            back_buf[step, :, r, :] = slots[r * group : (r + 1) * group]
        for d in order:
            group_copy(step, d, True).start()
        answer_buf[step, my_place] = back_buf[step, my_place]
        edge.wait_recv()
        internal = []
        for k in range(3):
            near = rim_send[step, pl.ds(k * 2, rows, stride=8), :]
            far = rim_send[step, pl.ds(k * 2 + 1, rows - 1, stride=8), :]
            edge_row = rim_recv[step, pl.ds(k * 2 + 1, 1), :]
            internal.append(near + jnp.concatenate([edge_row, far], axis=0))
        row_iota = lax.broadcasted_iota(jnp.int32, (rows, LANES), 0)
        for d in order[::-1]:
            group_copy(step, d, True).wait_recv()
        for g in range(group):
            for half in range(halves):
                high = slot_high[g, pl.ds(half, 1), :]
                match = row_iota == high
                chosen = jnp.concatenate([
                    jnp.where(
                        match,
                        jnp.broadcast_to(answer_buf[step, g, pl.ds(k * halves + half, 1), :], match.shape),
                        0.0,
                    )
                    for k in range(3)
                ], axis=0)
                first = chosen.astype(BF16).astype(F32)
                both = jnp.concatenate([first, chosen - first], axis=0).astype(BF16)
                node_lhs[:, pl.ds((g * halves + half) * LANES, LANES)] = both
        contact = nt_dot(node_lhs[...], node_hot[...])
        contact = contact[: 3 * rows] + contact[3 * rows :]
        for k in range(3):
            fresh = velocity_rows(k) + TIME_STEP * (
                internal[k] + contact[k * rows : (k + 1) * rows]
            ) / mass
            vel[pl.ds(k * 2 * rows, rows), :] = fresh
            pos[pl.ds(k * rows, rows), :] = pos[pl.ds(k * rows, rows), :] + TIME_STEP * fresh
        if step + 1 < STEPS:
            fill_ghosts(step + 1)
            fill_slots(step + 1)

    coords_out[...] = pos[...]
    for k in range(3):
        velocity_out[pl.ds(k * rows, rows), :] = velocity_rows(k)
    stress_out[...] = stress[...]
    for step in range(STEPS):
        edge_copy(step, 0).wait_send()
        pltpu.make_async_remote_copy(
            src_ref=rim_send.at[step, pl.ds((rows - 1) * 8, 8)], dst_ref=rim_recv.at[step],
            send_sem=edge_send_sem.at[step, 1], recv_sem=edge_recv_sem.at[step, 1],
            device_id=after, device_id_type=MESH,
        ).wait_send()
        for d in range(1, group):
            group_copy(step, d, False).wait_send()
            group_copy(step, d, True).wait_send()


def arrange(coords_rows, velocity_rows, stress_rows, coords_out, velocity_out, stress_out):
    rows = coords_rows.shape[0] // 3
    pairs = ((coords_rows, coords_out), (velocity_rows, velocity_out), (stress_rows, stress_out))
    for source, target in pairs:
        for i in range(rows):
            target[:, pl.ds(i * LANES, LANES)] = source[pl.ds(i, 3, stride=rows), :]


def per_device(
    sizes, coords, velocity, node_mass, corner_nodes, shape_grad, frame_angles, volume, stress,
    send_nodes, tile_count, tile_nodes, tile_facets, pair_mask,
):
    count = coords.shape[1]
    rows = count // LANES
    group = sizes[1] * sizes[2]
    cap = send_nodes.shape[2]
    tiles = tile_nodes.shape[0]
    spans = group * cap // LANES
    vmem = pl.BlockSpec(memory_space=pltpu.VMEM)
    smem = pl.BlockSpec(memory_space=pltpu.SMEM)
    state = jax.ShapeDtypeStruct((3, count), F32)
    packed = jax.ShapeDtypeStruct((3 * rows, LANES), F32)
    hbm = pl.BlockSpec(memory_space=pl.ANY)
    halves = cap // LANES
    arrays = (
        coords, velocity, node_mass.reshape(rows, LANES), corner_nodes, shape_grad, frame_angles,
        volume.reshape(rows, LANES), stress, send_nodes, tile_nodes, tile_facets, pair_mask,
    )
    dma = pltpu.SemaphoreType.DMA
    finals = pl.pallas_call(
        functools.partial(kernel, sizes),
        out_shape=(packed, packed, packed),
        in_specs=[hbm] * 9 + [smem] + [hbm] * 3,
        out_specs=(vmem, vmem, vmem),
        scratch_shapes=[pltpu.VMEM(a.shape, a.dtype) for a in arrays] + [
            dma((len(arrays),)),
            pltpu.VMEM((3 * rows, LANES), F32),
            pltpu.VMEM((6 * rows, LANES), F32),
            pltpu.VMEM((4 * rows, LANES), jnp.int32),
            pltpu.VMEM((8 * rows, LANES), F32),
            pltpu.VMEM((3 * rows, LANES), F32),
            pltpu.VMEM((2 * rows, LANES), F32),
            pltpu.VMEM((group, halves, LANES), jnp.int32),
            pltpu.VMEM((-(-5 * tiles // 8) * 8, LANES), jnp.int32),
            pltpu.VMEM((rows, LANES, 4 * LANES), BF16),
            pltpu.VMEM((LANES, 5 * tiles * LANES), BF16),
            pltpu.VMEM((LANES, group * cap), BF16),
            pltpu.VMEM((4, 16 * rows, LANES), F32),
            pltpu.VMEM((6 * spans, 5 * tiles * LANES), BF16),
            pltpu.VMEM((6 * rows, group * cap), BF16),
            pltpu.VMEM((group, 6 * halves, LANES), F32),
            pltpu.VMEM((group, 6 * halves, LANES), F32),
            pltpu.VMEM((STEPS - 1, group, 3 * halves, LANES), F32),
            pltpu.VMEM((STEPS - 1, group, 3 * halves, LANES), F32),
            pltpu.VMEM((STEPS, group, 3 * halves, LANES), F32),
            pltpu.VMEM((STEPS, group, 3 * halves, LANES), F32),
            pltpu.VMEM((STEPS, 3, LANES), F32),
            pltpu.VMEM((STEPS, 3, LANES), F32),
            pltpu.VMEM((STEPS, 8 * rows, LANES), F32),
            pltpu.VMEM((STEPS, 8, LANES), F32),
            dma((STEPS, group - 1)),
            dma((STEPS, group - 1)),
            dma((STEPS, group - 1)),
            dma((STEPS, group - 1)),
            dma((STEPS, 2)),
            dma((STEPS, 2)),
        ],
        compiler_params=pltpu.CompilerParams(collective_id=0, has_side_effects=True),
    )(*arrays[:9], tile_count, *arrays[9:])
    return pl.pallas_call(
        arrange,
        out_shape=(state, state, state),
        in_specs=[vmem] * 3,
        out_specs=(vmem, vmem, vmem),
    )(*finals)


def solution(mesh):
    axes = ("len", "wid", "dep")
    flat, wide = P(axes), P(None, axes)
    sizes = tuple(mesh.shape[name] for name in axes)
    return jax.shard_map(
        functools.partial(per_device, sizes),
        mesh=mesh,
        in_specs=(
            wide, wide, flat, wide, wide, wide, flat, wide,
            P(axes, None, None), flat, P(axes, None), P(None, axes, None), P(axes, None, None),
        ),
        out_specs=(wide, wide, wide),
        check_vma=False,
    )
```
